32 devices in a mesh: rep: 4 (over y, x), dom: 8 (over z, core).
Axes of the slice: x: 2, y: 2, z: 4, core: 2. Of those that a mesh axis runs over, the one named last changes fastest.
Arguments:
- node_pos: float32 [3, 16384], P(None, 'dom'), may hold values from -6 to 6
- node_order: int32 [8, 2048], P('dom'), may hold values from 0 to 2047, each once within a row
- facet_centroid: float32 [3, 16384], P(None, 'dom'), may hold values from -6 to 6
- facet_normal: float32 [3, 16384], P(None, 'dom'), may hold values from -6 to 6
- facet_nodes: int32 [3, 16384], P(None, 'dom'), may hold values from 0 to 2047
- pair_bucket: int32 [4, 8, 128], P('rep', 'dom'), may hold values from 0 to 15
- pair_owner: int32 [4, 8, 128, 1], P('rep', 'dom'), may hold values from 0 to 7; in each aligned block of 128 rows (0 to 127, 128 to 255, ..., all dimensions but the last counted through in order) at most 32 rows name the same one
- pair_slot: int32 [4, 8, 128], P('rep', 'dom'), may hold values from 0 to 15
- pair_count: int32 [4, 8], P('rep', 'dom'), may hold values from 64 to 128, as said below
Outputs:
- node_force: float32 [3, 16384], P(None, 'dom')
The draws below stay inside these ranges and needn't reach their ends.
Inputs may be any that keep to these rules, and one draw needn't show every extreme that they name: `pair_owner`: among the 128 pairs of one device, each domain is named at most 32 times, and exactly 32 times in some device's pairs. `pair_count`: some device uses all 128 pairs. `node_order`: each row is a permutation.
All inputs are finite; a program needn't handle non-finite values.
Results may differ from the reference program's by a relative error of at most 0.00013.
Values sent between devices are 32-bit elements; how exact they have to be, the bound alone decides.
A program may use at most 64 MiB of HBM per device.

```python
import math
import jax
import jax.numpy as jnp
import numpy as np
from jax import lax

BUCKET = 128
FB_DEV = 16
NB_DEV = 16
PAIRS_DEV = 128
CAP = 32
NODE_DEV = 2048
FACET_DEV = 2048
NODES = 16384
FACETS = 16384
N_REP = 4
N_DOM = 8


def draw_pair_count(key, part):
    halvings = jax.random.randint(jax.random.fold_in(key, 11), (N_REP, N_DOM), 0, 2)
    divisor = jnp.array([1, 2], jnp.int32)[halvings]
    counts = (PAIRS_DEV // divisor).astype(jnp.int32)
    full_rep = jax.random.randint(jax.random.fold_in(key, 12), (), 0, N_REP)
    full_dom = jax.random.randint(jax.random.fold_in(key, 13), (), 0, N_DOM)
    return counts.at[full_rep, full_dom].set(PAIRS_DEV)


def set_ends(result, key, smallest, top_value):
    longest = result.shape.index(max(result.shape))
    spots = []
    for shift in (0, 1):
        where = [jax.random.randint(jax.random.fold_in(key, axis), (), 0, length) for axis, length in enumerate(result.shape)]
        where[longest] = (where[longest] + shift) % result.shape[longest]
        spots.append(tuple(where))
    return result.at[spots[0]].set(smallest).at[spots[1]].set(top_value)


def levels(stream_key, dims, cuts, smallest, largest):
    gain = 1.0
    for axis_at, shards_of in cuts:
        steps = jax.random.uniform(jax.random.fold_in(jax.random.fold_in(stream_key, 6), axis_at), (shards_of,), jnp.float32, smallest / len(cuts), largest / len(cuts))
        gain = gain * jnp.repeat(jnp.exp(steps), dims[axis_at] // shards_of).reshape((-1,) + (1,) * (len(dims) - 1 - axis_at))
    return gain


def routed_block(key, own, number, rows, number_of, top, bound, slope):
    sequence = jax.random.permutation(key, number_of)
    crowded, usual = load_shares(number_of, rows * top, bound, slope, True), load_shares(number_of, rows * top, bound, slope, False)
    places = jnp.arange(number_of)

    def named(tallies, turn):
        used = int((tallies > 0).sum())
        fixed = max(1, used // 4)
        moved = fixed + (places - fixed + turn * (used - fixed)) % max(1, number_of - fixed)
        return jnp.zeros((number_of,), jnp.int32).at[sequence[jnp.where(places < fixed, places, moved)]].set(jnp.asarray(tallies, jnp.int32))

    tallies = jnp.where(number % 4 == 0, named(crowded, number // 4), named(usual, number - number // 4 - 1))
    mixed = jax.random.permutation(jax.random.fold_in(own, 3), number_of)
    giver, receiver = mixed[0:number_of // 2 * 2:2], mixed[1:number_of // 2 * 2:2]
    room = jnp.minimum(tallies[giver] - 1, bound - tallies[receiver]) // 2
    room = jnp.where((giver == sequence[0]) | (receiver == sequence[0]) | (tallies[receiver] == 0), 0, jnp.maximum(room, 0))
    moved = jax.random.randint(jax.random.fold_in(own, 4), (number_of // 2,), 0, 1 << 20) % (room + 1)
    tallies = tallies.at[giver].add(-moved).at[receiver].add(moved)
    items = jnp.searchsorted(jnp.cumsum(tallies), jnp.arange(rows * top), side="right").astype(jnp.int32)
    grid = items.reshape(top, rows).T
    grid = grid[jax.random.permutation(jax.random.fold_in(own, 1), rows)]
    turn = jax.random.randint(jax.random.fold_in(own, 2), (rows, 1), 0, top)
    return jnp.take_along_axis(grid, (jnp.arange(top)[None, :] + turn) % top, axis=1)


def load_shares(amount, total, bound, skew, full):
    portions = [(1 << 20) // math.isqrt(grade ** skew) + 1 for grade in range(1, amount + 1)]
    largest = bound if full else min(bound, max(-(-total // amount), total * portions[0] // sum(portions)))
    least = 1 if total - largest >= amount - 1 else 0
    given, surplus = [largest] + [least] * (amount - 1), total - largest - least * (amount - 1)
    while surplus > 0:
        candidates = [i for i in range(1, amount) if given[i] < largest] or [i for i in range(1, amount) if given[i] < bound]
        pool, left = sum([portions[i] for i in candidates]), surplus
        for i in candidates:
            extra = min(bound - given[i], max(1, left * portions[i] // pool), surplus)
            given[i] = given[i] + extra
            surplus = surplus - extra
    return np.array(given)


def noise(rng, extent, deviation, reach, shards=(), kind=jnp.bfloat16):
    result = jax.random.normal(rng, extent, jnp.float32) * deviation
    if len(shards) > 0:
        result = levels(rng, extent, shards, -0.22, 0.18) * result
    return jnp.clip(result, min=-reach, max=reach).astype(kind)


def setup_inputs(seed: int = 0) -> dict:
    streams_of = jax.random.split(jax.random.key(seed), 10)
    node_pos = noise(streams_of[0], (3, NODES), 1.0, 6.0, ((1, 8),), jnp.float32)
    node_order = jax.vmap(lambda own: jax.random.permutation(own, NODE_DEV))(jax.random.split(streams_of[1], N_DOM)).reshape((N_DOM, NODE_DEV)).astype(jnp.int32)
    facet_centroid = noise(streams_of[2], (3, FACETS), 1.0, 6.0, ((1, 8),), jnp.float32)
    facet_normal = noise(streams_of[3], (3, FACETS), 1.0, 6.0, ((1, 8),), jnp.float32)
    facet_nodes = set_ends(jax.random.randint(streams_of[4], (3, FACETS), 0, NODE_DEV), jax.random.fold_in(streams_of[4], 1), 0, NODE_DEV - 1).astype(jnp.int32)
    pair_bucket = set_ends(jax.random.randint(streams_of[5], (N_REP, N_DOM, PAIRS_DEV), 0, FB_DEV), jax.random.fold_in(streams_of[5], 1), 0, FB_DEV - 1).astype(jnp.int32)
    pair_owner_keys = jax.random.split(jax.random.fold_in(streams_of[6], 1), N_REP * N_DOM * PAIRS_DEV // PAIRS_DEV)
    pair_owner_turns = jax.random.permutation(jax.random.fold_in(streams_of[6], 3), N_REP * N_DOM * PAIRS_DEV // PAIRS_DEV)
    pair_owner = jax.vmap(lambda own, number: routed_block(jax.random.fold_in(streams_of[6], 2), own, number, PAIRS_DEV, N_DOM, 1, CAP, 2))(pair_owner_keys, pair_owner_turns).reshape((N_REP, N_DOM, PAIRS_DEV, 1))
    pair_slot = set_ends(jax.random.randint(streams_of[7], (N_REP, N_DOM, PAIRS_DEV), 0, NB_DEV), jax.random.fold_in(streams_of[7], 1), 0, NB_DEV - 1).astype(jnp.int32)
    pair_count = draw_pair_count(jax.random.fold_in(streams_of[9], 71), 0)
    return {"node_pos": node_pos, "node_order": node_order, "facet_centroid": facet_centroid, "facet_normal": facet_normal, "facet_nodes": facet_nodes, "pair_bucket": pair_bucket, "pair_owner": pair_owner, "pair_slot": pair_slot, "pair_count": pair_count}


STIFFNESS = 0.125
RADIUS_SQ = 4.0
ref_block = 64


def tile_terms(facet_geom, node_points):
    centre = facet_geom[:, 0:3]
    normal = facet_geom[:, 3:6]
    delta = node_points[:, :, None, :] - centre[:, :, :, None]
    gap = jnp.sum(normal[:, :, :, None] * delta, axis=1)
    dist = jnp.sum(delta * delta, axis=1)
    strength = STIFFNESS * jax.nn.softplus(-gap) * jnp.exp(-dist / RADIUS_SQ)
    node_term = jnp.einsum("bkf,bfp->bkp", normal, strength, precision=lax.Precision.HIGHEST)
    reaction = -normal * jnp.sum(strength, axis=2)[:, None, :]
    return node_term, reaction


def reference(node_pos, node_order, facet_centroid, facet_normal, facet_nodes, pair_bucket, pair_owner, pair_slot, pair_count):
    node_base = (jnp.arange(N_DOM, dtype=jnp.int32) * NODE_DEV)[:, None]
    global_order = (node_order + node_base).reshape(-1).astype(jnp.int32)
    bucketed = node_pos[:, global_order].reshape(3, N_DOM * NB_DEV, BUCKET).transpose(1, 0, 2)
    geometry = jnp.concatenate([facet_centroid, facet_normal], 0)
    geometry = geometry.reshape(6, N_DOM * FB_DEV, BUCKET).transpose(1, 0, 2)
    domain_ids = jnp.arange(N_DOM, dtype=jnp.int32)[None, :, None]
    facet_bucket = (domain_ids * FB_DEV + pair_bucket).reshape(-1).astype(jnp.int32)
    node_bucket = (pair_owner[:, :, :, 0] * NB_DEV + pair_slot).reshape(-1).astype(jnp.int32)
    is_live = (jnp.arange(PAIRS_DEV, dtype=jnp.int32)[None, None, :] < pair_count[:, :, None]).reshape(-1)
    sort_order = jnp.argsort(jnp.where(is_live, 0, 1).astype(jnp.int32), stable=True)
    live_count = jnp.sum(is_live.astype(jnp.int32))
    padding = jnp.zeros((ref_block,), jnp.int32)
    facet_rows = jnp.concatenate([facet_bucket[sort_order], padding])
    node_rows = jnp.concatenate([node_bucket[sort_order], padding])
    live_rows = jnp.concatenate([is_live[sort_order], padding > 0])

    def step(block_index, carry):
        node_acc, facet_acc = carry
        start = (block_index * ref_block).astype(jnp.int32)
        facet_take = lax.dynamic_slice_in_dim(facet_rows, start, ref_block)
        node_take = lax.dynamic_slice_in_dim(node_rows, start, ref_block)
        weight = lax.dynamic_slice_in_dim(live_rows, start, ref_block).astype(jnp.float32)
        node_term, reaction = tile_terms(geometry[facet_take], bucketed[node_take])
        node_acc = node_acc.at[node_take].add(node_term * weight[:, None, None])
        facet_acc = facet_acc.at[facet_take].add(reaction * weight[:, None, None])
        return node_acc, facet_acc

    blocks = (live_count + ref_block - 1) // ref_block
    start_acc = (jnp.zeros((N_DOM * NB_DEV, 3, BUCKET), jnp.float32), jnp.zeros((N_DOM * FB_DEV, 3, BUCKET), jnp.float32))
    node_acc, facet_acc = lax.fori_loop(jnp.int32(0), blocks.astype(jnp.int32), step, start_acc)
    node_flat = node_acc.transpose(1, 0, 2).reshape(3, N_DOM * NODE_DEV)
    node_force = jnp.zeros((3, N_DOM * NODE_DEV), jnp.float32).at[:, global_order].add(node_flat)
    reaction = facet_acc.transpose(1, 0, 2).reshape(3, N_DOM * FACET_DEV) / 3.0
    vertex_base = jnp.repeat(jnp.arange(N_DOM, dtype=jnp.int32) * NODE_DEV, FACET_DEV)
    for corner in range(3):
        node_force = node_force.at[:, (facet_nodes[corner] + vertex_base).astype(jnp.int32)].add(reaction)
    return node_force
```

```python
import functools

import jax
import jax.numpy as jnp
from jax import lax
from jax.experimental import pallas as pl
from jax.experimental.pallas import tpu as pltpu
from jax.sharding import PartitionSpec as P

BUCKET = 128
STIFFNESS = 0.125
RADIUS_SQ = 4.0
LOG2E = 1.4426950408889634
MESH_ID = pl.DeviceIdType.MESH
VMEM = pl.BlockSpec(memory_space=pltpu.VMEM)
SMEM = pl.BlockSpec(memory_space=pltpu.SMEM)
F32 = jnp.float32
BF16 = jnp.bfloat16


def repeat(count, body):
    if count <= 16:
        for i in range(count):
            body(i)
    else:
        def step(i, carry):
            body(i)
            return carry

        lax.fori_loop(0, count, step, 0)


def split3(value):
    first = value.astype(BF16).astype(F32)
    rest = value - first
    second = rest.astype(BF16).astype(F32)
    return first, second, rest - second


def gather_kernel(domains, pos_ref, order_ref, out_ref, send_sem, recv_sem):
    me = lax.axis_index("dom")
    rows = out_ref.shape[0] // domains
    buckets = rows // 3
    barrier = pltpu.get_barrier_semaphore()

    def greet(t):
        peer = lax.rem(me + t + 1, domains)
        pl.semaphore_signal(barrier, inc=1, device_id={"dom": peer}, device_id_type=MESH_ID)

    repeat(domains - 1, greet)

    order = jnp.concatenate(
        [order_ref[:, h * BUCKET : (h + 1) * BUCKET] for h in range(buckets)], 0
    )
    high = lax.div(order, BUCKET)
    low = order - high * BUCKET
    own = pl.multiple_of(me * rows, 8)
    for k in range(3):
        picked = jnp.zeros((buckets, BUCKET), F32)
        for h in range(buckets):
            row = jnp.broadcast_to(
                pos_ref[k : k + 1, h * BUCKET : (h + 1) * BUCKET], (buckets, BUCKET)
            )
            found = jnp.take_along_axis(row, low, axis=1, mode="promise_in_bounds")
            picked = jnp.where(high == h, found, picked)
        out_ref[pl.ds(own + k * buckets, buckets), :] = picked

    pl.semaphore_wait(barrier, domains - 1)
    block = out_ref.at[pl.ds(own, rows)]

    def copy_to(t):
        peer = lax.rem(me + t + 1, domains)
        return pltpu.make_async_remote_copy(
            src_ref=block,
            dst_ref=block,
            send_sem=send_sem.at[t],
            recv_sem=recv_sem.at[t],
            device_id={"dom": peer},
            device_id_type=MESH_ID,
        )

    def copy_from(t):
        source = lax.rem(me + 2 * domains - t - 1, domains)
        landed = out_ref.at[pl.ds(pl.multiple_of(source * rows, 8), rows)]
        return pltpu.make_async_remote_copy(
            src_ref=landed,
            dst_ref=landed,
            send_sem=send_sem.at[t],
            recv_sem=recv_sem.at[t],
            device_id={"dom": source},
            device_id_type=MESH_ID,
        )

    repeat(domains - 1, lambda t: copy_to(t).start())
    repeat(domains - 1, lambda t: copy_from(t).wait_recv())
    repeat(domains - 1, lambda t: copy_to(t).wait_send())


def pair_kernel(
    node_buckets,
    count_ref,
    bucket_ref,
    owner_ref,
    slot_ref,
    points_ref,
    centre_ref,
    normal_ref,
    nodes_ref,
    rows_ref,
    geom_ref,
    wide_ref,
    sum_ref,
):
    facet_buckets = centre_ref.shape[1] // BUCKET
    nodes_ref[...] = jnp.zeros_like(nodes_ref)
    sum_ref[...] = jnp.zeros_like(sum_ref)
    scale = LOG2E / RADIUS_SQ
    nothing = jnp.zeros((1, BUCKET), F32)

    def prepare(b, carry):
        at = pl.ds(pl.multiple_of(b * BUCKET, BUCKET), BUCKET)
        n = [normal_ref[k : k + 1, at] for k in range(3)]
        c = [centre_ref[k : k + 1, at] for k in range(3)]
        n_c = n[0] * c[0] + n[1] * c[1] + n[2] * c[2]
        c_c = c[0] * c[0] + c[1] * c[1] + c[2] * c[2]
        gap = jnp.concatenate([-n[0], -n[1], -n[2], nothing, n_c] + [nothing] * 3, 0)
        dist = jnp.concatenate(
            [2.0 * scale * c[0], 2.0 * scale * c[1], 2.0 * scale * c[2]]
            + [nothing - scale, -scale * c_c] + [nothing] * 3,
            0,
        )
        raw = jnp.concatenate(n + [nothing] * 5, 0)
        blank = jnp.zeros((BUCKET - 56, BUCKET), F32)
        for part, rows in enumerate((gap, dist)):
            a, bb, cc = split3(rows)
            table = jnp.concatenate([a, bb, cc, a, bb, a, raw, blank], 0).T
            geom_ref[b, part * BUCKET : (part + 1) * BUCKET, :] = table.astype(BF16)
            if part == 0:
                for k in range(3):
                    wide_ref[b, k] = jnp.broadcast_to(table[:, 48 + k : 49 + k], (BUCKET, BUCKET))
        return carry

    lax.fori_loop(0, facet_buckets, prepare, 0)

    count = count_ref[0, 0]
    place = lax.broadcasted_iota(jnp.int32, (8, BUCKET), 0)
    blank = jnp.zeros((BUCKET - 48, BUCKET), F32)
    spare = nodes_ref.shape[0] - 3 * node_buckets

    def one(p):
        live = p < count
        b = bucket_ref[p]
        base = owner_ref[p] * (3 * node_buckets) + slot_ref[p]
        x, y, z = (
            jnp.broadcast_to(points_ref[pl.ds(base + k * node_buckets, 1), :], (8, BUCKET))
            for k in range(3)
        )
        square = x * x + y * y + z * z
        one_or_zero = jnp.where(place == 4, 1.0, 0.0)
        value = jnp.where(place == 3, square, one_or_zero)
        value = jnp.where(place == 2, z, value)
        value = jnp.where(place == 1, y, value)
        value = jnp.where(place == 0, x, value)
        v1, v2, v3 = split3(value)
        table = jnp.concatenate([v1, v1, v1, v2, v2, v3, blank], 0).astype(BF16)
        both = jnp.dot(geom_ref[b], table, preferred_element_type=F32)
        minus_gap, fade = both[:BUCKET], both[BUCKET:]
        small = jnp.exp(-jnp.abs(minus_gap))
        logs = jnp.where(small < 2.0**-8, small * (1.0 - 0.5 * small), jnp.log(1.0 + small))
        strength = (jnp.maximum(minus_gap, 0.0) + logs) * jnp.exp2(fade)
        to_bucket = jnp.where(live, b, facet_buckets)
        to_node = jnp.where(live, base, spare)
        sum_ref[to_bucket] += strength
        for k in range(3):
            term = jnp.sum(wide_ref[b, k] * strength, axis=0, keepdims=True)
            nodes_ref[pl.ds(to_node + k * node_buckets, 1), :] += term

    def step(i, carry):
        one(2 * i)
        one(2 * i + 1)
        return carry

    lax.fori_loop(0, lax.div(count + 1, 2), step, 0)

    for b in range(facet_buckets):
        rows_ref[b : b + 1, :] = jnp.sum(sum_ref[b].T, axis=0, keepdims=True)


def exchange_kernel(
    domains,
    copies,
    nodes_ref,
    rows_ref,
    nodes_out,
    rows_out,
    landed,
    landed_rows,
    total,
    landed_total,
    send_sem,
    recv_sem,
    send_row,
    recv_row,
    send_total,
    recv_total,
):
    me = lax.axis_index("dom")
    rep = lax.axis_index("rep")
    size = landed.shape[1]
    barrier = pltpu.get_barrier_semaphore()

    def dom_peer(t):
        return lax.rem(me + t + 1, domains)

    def rep_peer(t):
        return lax.rem(rep + t + 1, copies)

    def signal(where):
        pl.semaphore_signal(barrier, inc=1, device_id=where, device_id_type=MESH_ID)

    repeat(domains - 1, lambda t: signal({"dom": dom_peer(t)}))
    repeat(copies - 1, lambda t: signal({"rep": rep_peer(t)}))
    pl.semaphore_wait(barrier, domains + copies - 2)

    def copy(src, dst, send, recv, where):
        return pltpu.make_async_remote_copy(
            src_ref=src,
            dst_ref=dst,
            send_sem=send,
            recv_sem=recv,
            device_id=where,
            device_id_type=MESH_ID,
        )

    def node_copy(t):
        block = nodes_ref.at[pl.ds(pl.multiple_of(dom_peer(t) * size, 8), size)]
        return copy(
            block, landed.at[t], send_sem.at[t], recv_sem.at[t], {"dom": dom_peer(t)}
        )

    def row_copy(t):
        return copy(
            rows_ref, landed_rows.at[t], send_row.at[t], recv_row.at[t], {"rep": rep_peer(t)}
        )

    def total_copy(t):
        return copy(
            total, landed_total.at[t], send_total.at[t], recv_total.at[t], {"rep": rep_peer(t)}
        )

    repeat(domains - 1, lambda t: node_copy(t).start())
    repeat(copies - 1, lambda t: row_copy(t).start())

    repeat(domains - 1, lambda t: node_copy(t).wait_recv())
    mine = nodes_ref[pl.ds(pl.multiple_of(me * size, 8), size), :]
    if domains <= 16:
        for t in range(domains - 1):
            mine = mine + landed[t]
    else:
        mine = lax.fori_loop(0, domains - 1, lambda t, s: s + landed[t], mine)
    total[...] = mine
    repeat(copies - 1, lambda t: row_copy(t).wait_recv())
    rows = rows_ref[...]
    for t in range(copies - 1):
        rows = rows + landed_rows[t]
    rows_out[...] = rows
    repeat(copies - 1, lambda t: total_copy(t).start())
    repeat(domains - 1, lambda t: node_copy(t).wait_send())
    repeat(copies - 1, lambda t: row_copy(t).wait_send())
    repeat(copies - 1, lambda t: total_copy(t).wait_recv())
    for t in range(copies - 1):
        mine = mine + landed_total[t]
    nodes_out[...] = mine
    repeat(copies - 1, lambda t: total_copy(t).wait_send())


def finish_kernel(nodes_ref, rows_ref, normal_ref, order_ref, corner_ref, out_ref):
    node_buckets = nodes_ref.shape[0] // 3
    facet_buckets = rows_ref.shape[0]
    high_at = lax.broadcasted_iota(jnp.int32, (node_buckets, BUCKET), 0)
    low_at = lax.broadcasted_iota(jnp.int32, (BUCKET, BUCKET), 0)
    result = jnp.zeros((6 * node_buckets, BUCKET), F32)

    def spread(index, values, result):
        high = lax.div(index, BUCKET)
        low = index - high * BUCKET
        hit = high == high_at
        onehot = jnp.where(low == low_at, 1.0, 0.0).astype(BF16)
        firsts = [v.astype(BF16).astype(F32) for v in values]
        rests = [v - f for v, f in zip(values, firsts)]
        left = jnp.concatenate([jnp.where(hit, v, 0.0) for v in firsts + rests], 0)
        return result + lax.dot_general(
            left.astype(BF16), onehot, (((1,), (1,)), ((), ())), preferred_element_type=F32
        )

    for j in range(node_buckets):
        values = [
            STIFFNESS * nodes_ref[k * node_buckets + j : k * node_buckets + j + 1, :]
            for k in range(3)
        ]
        result = spread(order_ref[:, j * BUCKET : (j + 1) * BUCKET], values, result)
    for b in range(facet_buckets):
        at = slice(b * BUCKET, (b + 1) * BUCKET)
        row = (-STIFFNESS / 3.0) * rows_ref[b : b + 1, :]
        values = [normal_ref[k : k + 1, at] * row for k in range(3)]
        for corner in range(3):
            result = spread(corner_ref[corner : corner + 1, at], values, result)

    half = 3 * node_buckets
    force = result[:half] + result[half:]
    for k in range(3):
        for h in range(node_buckets):
            i = k * node_buckets + h
            out_ref[k : k + 1, h * BUCKET : (h + 1) * BUCKET] = force[i : i + 1]


def per_device(
    node_pos,
    node_order,
    facet_centroid,
    facet_normal,
    facet_nodes,
    pair_bucket,
    pair_owner,
    pair_slot,
    pair_count,
):
    domains = lax.axis_size("dom")
    copies = lax.axis_size("rep")
    node_buckets = node_pos.shape[1] // BUCKET
    facet_buckets = facet_centroid.shape[1] // BUCKET
    size = 3 * node_buckets
    dma = pltpu.SemaphoreType.DMA
    shape = jax.ShapeDtypeStruct

    points = pl.pallas_call(
        functools.partial(gather_kernel, domains),
        name="gather_points",
        out_shape=shape((domains * size, BUCKET), F32),
        in_specs=[VMEM] * 2,
        out_specs=VMEM,
        scratch_shapes=[dma((domains - 1,)), dma((domains - 1,))],
        compiler_params=pltpu.CompilerParams(collective_id=0, has_side_effects=True),
    )(node_pos, node_order)

    nodes, rows = pl.pallas_call(
        functools.partial(pair_kernel, node_buckets),
        name="pair_forces",
        out_shape=[
            shape(((domains + 1) * size, BUCKET), F32),
            shape((facet_buckets, BUCKET), F32),
        ],
        in_specs=[SMEM] * 4 + [VMEM] * 3,
        out_specs=[VMEM] * 2,
        scratch_shapes=[
            pltpu.VMEM((facet_buckets, 2 * BUCKET, BUCKET), BF16),
            pltpu.VMEM((facet_buckets, 3, BUCKET, BUCKET), F32),
            pltpu.VMEM((facet_buckets + 1, BUCKET, BUCKET), F32),
        ],
    )(
        pair_count,
        pair_bucket.reshape(-1),
        pair_owner.reshape(-1),
        pair_slot.reshape(-1),
        points,
        facet_centroid,
        facet_normal,
    )

    nodes, rows = pl.pallas_call(
        functools.partial(exchange_kernel, domains, copies),
        name="exchange_forces",
        out_shape=[shape((size, BUCKET), F32), shape((facet_buckets, BUCKET), F32)],
        in_specs=[VMEM] * 2,
        out_specs=[VMEM] * 2,
        scratch_shapes=[
            pltpu.VMEM((domains - 1, size, BUCKET), F32),
            pltpu.VMEM((copies - 1, facet_buckets, BUCKET), F32),
            pltpu.VMEM((size, BUCKET), F32),
            pltpu.VMEM((copies - 1, size, BUCKET), F32),
            dma((domains - 1,)),
            dma((domains - 1,)),
            dma((copies - 1,)),
            dma((copies - 1,)),
            dma((copies - 1,)),
            dma((copies - 1,)),
        ],
        compiler_params=pltpu.CompilerParams(collective_id=1, has_side_effects=True),
    )(nodes, rows)

    return pl.pallas_call(
        finish_kernel,
        name="finish_forces",
        out_shape=shape(node_pos.shape, F32),
        in_specs=[VMEM] * 5,
        out_specs=VMEM,
    )(nodes, rows, facet_normal, node_order, facet_nodes)


def solution(mesh):
    placed = (
        P(None, "dom"),
        P("dom", None),
        P(None, "dom"),
        P(None, "dom"),
        P(None, "dom"),
        P("rep", "dom", None),
        P("rep", "dom", None, None),
        P("rep", "dom", None),
        P("rep", "dom"),
    )
    return jax.shard_map(
        per_device, mesh=mesh, in_specs=placed, out_specs=P(None, "dom"), check_vma=False
    )
```

```python
import functools

import jax
import jax.numpy as jnp
from jax import lax
from jax.experimental import pallas as pl
from jax.experimental.pallas import tpu as pltpu
from jax.sharding import PartitionSpec as P

BUCKET = 128
STIFFNESS = 0.125
RADIUS_SQ = 4.0
LOG2E = 1.4426950408889634
MESH_ID = pl.DeviceIdType.MESH
VMEM = pl.BlockSpec(memory_space=pltpu.VMEM)
SMEM = pl.BlockSpec(memory_space=pltpu.SMEM)
F32 = jnp.float32
BF16 = jnp.bfloat16


def repeat(count, body):
    if count <= 16:
        for i in range(count):
            body(i)
    else:
        def step(i, carry):
            body(i)
            return carry

        lax.fori_loop(0, count, step, 0)


def split3(value):
    first = value.astype(BF16).astype(F32)
    rest = value - first
    second = rest.astype(BF16).astype(F32)
    return first, second, rest - second


def facet_tables(centre_ref, normal_ref, geom_ref, wide_ref):
    scale = LOG2E / RADIUS_SQ
    nothing = jnp.zeros((1, BUCKET), F32)

    def prepare(b, carry):
        at = pl.ds(pl.multiple_of(b * BUCKET, BUCKET), BUCKET)
        n = [normal_ref[k : k + 1, at] for k in range(3)]
        c = [centre_ref[k : k + 1, at] for k in range(3)]
        n_c = n[0] * c[0] + n[1] * c[1] + n[2] * c[2]
        c_c = c[0] * c[0] + c[1] * c[1] + c[2] * c[2]
        gap = jnp.concatenate([-n[0], -n[1], -n[2], nothing, n_c] + [nothing] * 3, 0)
        dist = jnp.concatenate(
            [2.0 * scale * c[0], 2.0 * scale * c[1], 2.0 * scale * c[2]]
            + [nothing - scale, -scale * c_c] + [nothing] * 3,
            0,
        )
        raw = jnp.concatenate(n + [nothing] * 5, 0)
        blank = jnp.zeros((BUCKET - 56, BUCKET), F32)
        for part, rows in enumerate((gap, dist)):
            a, bb, cc = split3(rows)
            table = jnp.concatenate([a, bb, cc, a, bb, a, raw, blank], 0).T
            geom_ref[b, part * BUCKET : (part + 1) * BUCKET, :] = table.astype(BF16)
            if part == 0:
                for k in range(3):
                    wide_ref[b, k] = jnp.broadcast_to(table[:, 48 + k : 49 + k], (BUCKET, BUCKET))
        return carry

    lax.fori_loop(0, geom_ref.shape[0], prepare, 0)


def gather_kernel(
    domains,
    pos_ref,
    order_ref,
    centre_ref,
    normal_ref,
    out_ref,
    geom_ref,
    wide_ref,
    send_sem,
    recv_sem,
):
    me = lax.axis_index("dom")
    rows = out_ref.shape[0] // domains
    buckets = rows // 3
    barrier = pltpu.get_barrier_semaphore()

    def greet(t):
        peer = lax.rem(me + t + 1, domains)
        pl.semaphore_signal(barrier, inc=1, device_id={"dom": peer}, device_id_type=MESH_ID)

    repeat(domains - 1, greet)

    order = jnp.concatenate(
        [order_ref[:, h * BUCKET : (h + 1) * BUCKET] for h in range(buckets)], 0
    )
    high = lax.div(order, BUCKET)
    low = order - high * BUCKET
    own = pl.multiple_of(me * rows, 8)
    for k in range(3):
        picked = jnp.zeros((buckets, BUCKET), F32)
        for h in range(buckets):
            row = jnp.broadcast_to(
                pos_ref[k : k + 1, h * BUCKET : (h + 1) * BUCKET], (buckets, BUCKET)
            )
            found = jnp.take_along_axis(row, low, axis=1, mode="promise_in_bounds")
            picked = jnp.where(high == h, found, picked)
        out_ref[pl.ds(own + k * buckets, buckets), :] = picked

    pl.semaphore_wait(barrier, domains - 1)
    block = out_ref.at[pl.ds(own, rows)]

    def copy_to(t):
        peer = lax.rem(me + t + 1, domains)
        return pltpu.make_async_remote_copy(
            src_ref=block,
            dst_ref=block,
            send_sem=send_sem.at[t],
            recv_sem=recv_sem.at[t],
            device_id={"dom": peer},
            device_id_type=MESH_ID,
        )

    def copy_from(t):
        source = lax.rem(me + 2 * domains - t - 1, domains)
        landed = out_ref.at[pl.ds(pl.multiple_of(source * rows, 8), rows)]
        return pltpu.make_async_remote_copy(
            src_ref=landed,
            dst_ref=landed,
            send_sem=send_sem.at[t],
            recv_sem=recv_sem.at[t],
            device_id={"dom": source},
            device_id_type=MESH_ID,
        )

    repeat(domains - 1, lambda t: copy_to(t).start())
    facet_tables(centre_ref, normal_ref, geom_ref, wide_ref)
    repeat(domains - 1, lambda t: copy_from(t).wait_recv())
    repeat(domains - 1, lambda t: copy_to(t).wait_send())


def pair_kernel(
    node_buckets,
    count_ref,
    bucket_ref,
    owner_ref,
    slot_ref,
    points_ref,
    geom_ref,
    wide_ref,
    nodes_ref,
    rows_ref,
    odd_ref,
    even_sum,
    odd_sum,
    even_part,
    odd_part,
):
    facet_buckets = geom_ref.shape[0]
    slots = bucket_ref.shape[0]
    for ref in (nodes_ref, odd_ref, even_sum, odd_sum):
        ref[...] = jnp.zeros_like(ref)

    count = count_ref[0, 0]
    place = lax.broadcasted_iota(jnp.int32, (8, BUCKET), 0)
    blank = jnp.zeros((BUCKET - 48, BUCKET), F32)
    one_or_zero = jnp.where(place == 4, 1.0, 0.0)
    spare = nodes_ref.shape[0] - 3 * node_buckets

    def base_of(p):
        return owner_ref[p] * (3 * node_buckets) + slot_ref[p]

    def products(p, part_ref):
        base = base_of(p)
        x, y, z = (
            jnp.broadcast_to(points_ref[pl.ds(base + k * node_buckets, 1), :], (8, BUCKET))
            for k in range(3)
        )
        square = x * x + y * y + z * z
        value = jnp.where(place == 3, square, one_or_zero)
        value = jnp.where(place == 2, z, value)
        value = jnp.where(place == 1, y, value)
        value = jnp.where(place == 0, x, value)
        v1, v2, v3 = split3(value)
        table = jnp.concatenate([v1, v1, v1, v2, v2, v3, blank], 0).astype(BF16)
        part_ref[...] = jnp.dot(geom_ref[bucket_ref[p]], table, preferred_element_type=F32)

    def forces(p, part_ref, force_ref, sum_ref):
        live = p < count
        at = jnp.minimum(p, slots - 1)
        b = bucket_ref[at]
        minus_gap, fade = part_ref[:BUCKET], part_ref[BUCKET:]
        small = jnp.exp(-jnp.abs(minus_gap))
        logs = jnp.where(small < 2.0**-8, small * (1.0 - 0.5 * small), jnp.log(1.0 + small))
        strength = (jnp.maximum(minus_gap, 0.0) + logs) * jnp.exp2(fade)
        to_bucket = jnp.where(live, b, facet_buckets)
        to_node = jnp.where(live, base_of(at), spare)
        sum_ref[to_bucket] += strength
        for k in range(3):
            term = jnp.sum(wide_ref[b, k] * strength, axis=0, keepdims=True)
            force_ref[pl.ds(to_node + k * node_buckets, 1), :] += term

    products(0, even_part)

    def step(i, carry):
        p = 2 * i
        last = slots - 1
        products(jnp.minimum(p + 1, last), odd_part)
        forces(p, even_part, nodes_ref, even_sum)
        products(jnp.minimum(p + 2, last), even_part)
        forces(p + 1, odd_part, odd_ref, odd_sum)
        return carry

    lax.fori_loop(0, lax.div(count + 1, 2), step, 0)

    nodes_ref[...] += odd_ref[...]
    for b in range(facet_buckets):
        rows_ref[b : b + 1, :] = jnp.sum((even_sum[b] + odd_sum[b]).T, axis=0, keepdims=True)


def spread(index, values, result):
    node_buckets = result.shape[0] // 6
    high_at = lax.broadcasted_iota(jnp.int32, (node_buckets, BUCKET), 0)
    low_at = lax.broadcasted_iota(jnp.int32, (BUCKET, BUCKET), 0)
    high = lax.div(index, BUCKET)
    low = index - high * BUCKET
    hit = high == high_at
    onehot = jnp.where(low == low_at, 1.0, 0.0).astype(BF16)
    firsts = [v.astype(BF16).astype(F32) for v in values]
    rests = [v - f for v, f in zip(values, firsts)]
    left = jnp.concatenate([jnp.where(hit, v, 0.0) for v in firsts + rests], 0)
    return result + lax.dot_general(
        left.astype(BF16), onehot, (((1,), (1,)), ((), ())), preferred_element_type=F32
    )


def exchange_kernel(
    domains,
    copies,
    nodes_ref,
    rows_ref,
    normal_ref,
    order_ref,
    corner_ref,
    out_ref,
    landed,
    total,
    landed_total,
    send_sem,
    recv_sem,
    send_total,
    recv_total,
):
    me = lax.axis_index("dom")
    rep = lax.axis_index("rep")
    size = landed.shape[1]
    node_buckets = size // 3
    facet_buckets = rows_ref.shape[0]
    barrier = pltpu.get_barrier_semaphore()

    def dom_peer(t):
        return lax.rem(me + t + 1, domains)

    def rep_peer(t):
        return lax.rem(rep + t + 1, copies)

    def signal(where):
        pl.semaphore_signal(barrier, inc=1, device_id=where, device_id_type=MESH_ID)

    repeat(domains - 1, lambda t: signal({"dom": dom_peer(t)}))
    repeat(copies - 1, lambda t: signal({"rep": rep_peer(t)}))
    pl.semaphore_wait(barrier, domains + copies - 2)

    def copy(src, dst, send, recv, where):
        return pltpu.make_async_remote_copy(
            src_ref=src,
            dst_ref=dst,
            send_sem=send,
            recv_sem=recv,
            device_id=where,
            device_id_type=MESH_ID,
        )

    def node_copy(t):
        block = nodes_ref.at[pl.ds(pl.multiple_of(dom_peer(t) * size, 8), size)]
        return copy(
            block, landed.at[t], send_sem.at[t], recv_sem.at[t], {"dom": dom_peer(t)}
        )

    def total_copy(t):
        return copy(
            total, landed_total.at[t], send_total.at[t], recv_total.at[t], {"rep": rep_peer(t)}
        )

    repeat(domains - 1, lambda t: node_copy(t).start())

    result = jnp.zeros((2 * size, BUCKET), F32)
    for b in range(facet_buckets):
        at = slice(b * BUCKET, (b + 1) * BUCKET)
        row = (-STIFFNESS / 3.0) * rows_ref[b : b + 1, :]
        values = [normal_ref[k : k + 1, at] * row for k in range(3)]
        for corner in range(3):
            result = spread(corner_ref[corner : corner + 1, at], values, result)

    repeat(domains - 1, lambda t: node_copy(t).wait_recv())
    mine = nodes_ref[pl.ds(pl.multiple_of(me * size, 8), size), :]
    if domains <= 16:
        for t in range(domains - 1):
            mine = mine + landed[t]
    else:
        mine = lax.fori_loop(0, domains - 1, lambda t, s: s + landed[t], mine)
    mine = STIFFNESS * mine
    for j in range(node_buckets):
        values = [
            mine[k * node_buckets + j : k * node_buckets + j + 1, :] for k in range(3)
        ]
        result = spread(order_ref[:, j * BUCKET : (j + 1) * BUCKET], values, result)
    force = result[:size] + result[size:]
    total[...] = force
    repeat(domains - 1, lambda t: node_copy(t).wait_send())
    repeat(copies - 1, lambda t: total_copy(t).start())
    repeat(copies - 1, lambda t: total_copy(t).wait_recv())
    for t in range(copies - 1):
        force = force + landed_total[t]
    for k in range(3):
        for h in range(node_buckets):
            i = k * node_buckets + h
            out_ref[k : k + 1, h * BUCKET : (h + 1) * BUCKET] = force[i : i + 1]
    repeat(copies - 1, lambda t: total_copy(t).wait_send())


def per_device(
    node_pos,
    node_order,
    facet_centroid,
    facet_normal,
    facet_nodes,
    pair_bucket,
    pair_owner,
    pair_slot,
    pair_count,
):
    domains = lax.axis_size("dom")
    copies = lax.axis_size("rep")
    node_buckets = node_pos.shape[1] // BUCKET
    facet_buckets = facet_centroid.shape[1] // BUCKET
    size = 3 * node_buckets
    dma = pltpu.SemaphoreType.DMA
    shape = jax.ShapeDtypeStruct

    points, geom, wide = pl.pallas_call(
        functools.partial(gather_kernel, domains),
        name="gather_points",
        out_shape=[
            shape((domains * size, BUCKET), F32),
            shape((facet_buckets, 2 * BUCKET, BUCKET), BF16),
            shape((facet_buckets, 3, BUCKET, BUCKET), F32),
        ],
        in_specs=[VMEM] * 4,
        out_specs=[VMEM] * 3,
        scratch_shapes=[dma((domains - 1,)), dma((domains - 1,))],
        compiler_params=pltpu.CompilerParams(
            collective_id=0, has_side_effects=True, vmem_limit_bytes=16 << 20
        ),
    )(node_pos, node_order, facet_centroid, facet_normal)

    nodes, rows = pl.pallas_call(
        functools.partial(pair_kernel, node_buckets),
        name="pair_forces",
        out_shape=[
            shape(((domains + 1) * size, BUCKET), F32),
            shape((facet_buckets, BUCKET), F32),
        ],
        in_specs=[SMEM] * 4 + [VMEM] * 3,
        out_specs=[VMEM] * 2,
        scratch_shapes=[
            pltpu.VMEM(((domains + 1) * size, BUCKET), F32),
            pltpu.VMEM((facet_buckets + 1, BUCKET, BUCKET), F32),
            pltpu.VMEM((facet_buckets + 1, BUCKET, BUCKET), F32),
            pltpu.VMEM((2 * BUCKET, BUCKET), F32),
            pltpu.VMEM((2 * BUCKET, BUCKET), F32),
        ],
        compiler_params=pltpu.CompilerParams(vmem_limit_bytes=32 << 20),
    )(
        pair_count,
        pair_bucket.reshape(-1),
        pair_owner.reshape(-1),
        pair_slot.reshape(-1),
        points,
        geom,
        wide,
    )

    return pl.pallas_call(
        functools.partial(exchange_kernel, domains, copies),
        name="exchange_forces",
        out_shape=shape(node_pos.shape, F32),
        in_specs=[VMEM] * 5,
        out_specs=VMEM,
        scratch_shapes=[
            pltpu.VMEM((domains - 1, size, BUCKET), F32),
            pltpu.VMEM((size, BUCKET), F32),
            pltpu.VMEM((copies - 1, size, BUCKET), F32),
            dma((domains - 1,)),
            dma((domains - 1,)),
            dma((copies - 1,)),
            dma((copies - 1,)),
        ],
        compiler_params=pltpu.CompilerParams(
            collective_id=1, has_side_effects=True, vmem_limit_bytes=16 << 20
        ),
    )(nodes, rows, facet_normal, node_order, facet_nodes)


def solution(mesh):
    placed = (
        P(None, "dom"),
        P("dom", None),
        P(None, "dom"),
        P(None, "dom"),
        P(None, "dom"),
        P("rep", "dom", None),
        P("rep", "dom", None, None),
        P("rep", "dom", None),
        P("rep", "dom"),
    )
    return jax.shard_map(
        per_device, mesh=mesh, in_specs=placed, out_specs=P(None, "dom"), check_vma=False
    )
```

```python
import functools

import jax
import jax.numpy as jnp
from jax import lax
from jax.experimental import pallas as pl
from jax.experimental.pallas import tpu as pltpu
from jax.sharding import PartitionSpec as P

BUCKET = 128
STIFFNESS = 0.125
RADIUS_SQ = 4.0
LOG2E = 1.4426950408889634
MESH_ID = pl.DeviceIdType.MESH
VMEM = pl.BlockSpec(memory_space=pltpu.VMEM)
SMEM = pl.BlockSpec(memory_space=pltpu.SMEM)
HBM = pl.BlockSpec(memory_space=pltpu.HBM)
F32 = jnp.float32
BF16 = jnp.bfloat16


def repeat(count, body):
    if count <= 16:
        for i in range(count):
            body(i)
    else:
        def step(i, carry):
            body(i)
            return carry

        lax.fori_loop(0, count, step, 0)


def across(me, mask, domains):
    peer = me
    bit = 1
    while bit < domains:
        peer = peer + bit * ((mask // bit) % 2) * (1 - 2 * ((me // bit) % 2))
        bit *= 2
    return peer


def split3(value):
    first = value.astype(BF16).astype(F32)
    rest = value - first
    second = rest.astype(BF16).astype(F32)
    return first, second, rest - second


def facet_tables(centre_ref, normal_ref, geom_ref, wide_ref, begin, end):
    scale = LOG2E / RADIUS_SQ
    nothing = jnp.zeros((1, BUCKET), F32)

    def prepare(b, carry):
        at = pl.ds(pl.multiple_of(b * BUCKET, BUCKET), BUCKET)
        n = [normal_ref[k : k + 1, at] for k in range(3)]
        c = [centre_ref[k : k + 1, at] for k in range(3)]
        n_c = n[0] * c[0] + n[1] * c[1] + n[2] * c[2]
        c_c = c[0] * c[0] + c[1] * c[1] + c[2] * c[2]
        gap = jnp.concatenate([-n[0], -n[1], -n[2], nothing, n_c] + [nothing] * 3, 0)
        dist = jnp.concatenate(
            [2.0 * scale * c[0], 2.0 * scale * c[1], 2.0 * scale * c[2]]
            + [nothing - scale, -scale * c_c] + [nothing] * 3,
            0,
        )
        raw = jnp.concatenate(n + [nothing] * 5, 0)
        blank = jnp.zeros((BUCKET - 104, BUCKET), F32)
        rows = []
        for part in (gap, dist):
            first, second, third = split3(part)
            rows += [first, second, third, first, second, first]
        table = jnp.concatenate(rows + [raw, blank], 0).T
        geom_ref[b] = table.astype(BF16)
        for k in range(3):
            wide_ref[b, k] = jnp.broadcast_to(table[:, 96 + k : 97 + k], (BUCKET, BUCKET))
        return carry

    lax.fori_loop(begin, end, prepare, 0)


def gather_kernel(
    domains,
    pos_hbm,
    order_hbm,
    centre_hbm,
    normal_hbm,
    out_ref,
    geom_ref,
    wide_ref,
    pos_ref,
    order_ref,
    centre_ref,
    normal_ref,
    load_sem,
    send_sem,
    recv_sem,
):
    me = lax.axis_index("dom")
    rows = out_ref.shape[0] // domains
    buckets = rows // 3
    loads = [
        pltpu.make_async_copy(src, dst, load_sem.at[i])
        for i, (src, dst) in enumerate(
            (
                (pos_hbm, pos_ref),
                (order_hbm, order_ref),
                (centre_hbm, centre_ref),
                (normal_hbm, normal_ref),
            )
        )
    ]
    for load in loads:
        load.start()
    barrier = pltpu.get_barrier_semaphore()
    far = domains // 2 - 1
    partner = across(me, 1, domains)

    def far_mask(t):
        return domains - 2 - 2 * t

    def greet(where):
        pl.semaphore_signal(barrier, inc=1, device_id={"dom": where}, device_id_type=MESH_ID)

    repeat(far, lambda t: greet(across(me, far_mask(t), domains)))
    greet(partner)
    loads[0].wait()
    loads[1].wait()

    order = jnp.concatenate(
        [order_ref[:, h * BUCKET : (h + 1) * BUCKET] for h in range(buckets)], 0
    )
    high = lax.div(order, BUCKET)
    low = order - high * BUCKET

    def block_of(domain):
        return out_ref.at[pl.ds(pl.multiple_of(domain * rows, 8), rows)]

    own = pl.multiple_of(me * rows, 8)
    for k in range(3):
        picked = jnp.zeros((buckets, BUCKET), F32)
        for h in range(buckets):
            row = jnp.broadcast_to(
                pos_ref[k : k + 1, h * BUCKET : (h + 1) * BUCKET], (buckets, BUCKET)
            )
            found = jnp.take_along_axis(row, low, axis=1, mode="promise_in_bounds")
            picked = jnp.where(high == h, found, picked)
        out_ref[pl.ds(own + k * buckets, buckets), :] = picked

    pl.semaphore_wait(barrier, far + 1)

    def copy(domain, number, where):
        return pltpu.make_async_remote_copy(
            src_ref=block_of(domain),
            dst_ref=block_of(domain),
            send_sem=send_sem.at[number],
            recv_sem=recv_sem.at[number],
            device_id={"dom": where},
            device_id_type=MESH_ID,
        )

    def far_copy(t):
        return copy(me, t, across(me, far_mask(t), domains))

    def far_landed(t):
        where = across(me, far_mask(t), domains)
        return copy(where, t, where)

    def pass_on(t):
        return copy(across(me, far_mask(t), domains), far + t, partner)

    def passed_landed(t):
        return copy(across(partner, far_mask(t), domains), far + t, partner)

    repeat(far, lambda t: far_copy(t).start())
    copy(me, 2 * far, partner).start()
    loads[2].wait()
    loads[3].wait()
    facet_tables(centre_ref, normal_ref, geom_ref, wide_ref, 0, geom_ref.shape[0] // 2)

    def forward(t):
        far_landed(far - 1 - t).wait_recv()
        pass_on(far - 1 - t).start()

    repeat(far, forward)
    facet_tables(
        centre_ref, normal_ref, geom_ref, wide_ref, geom_ref.shape[0] // 2, geom_ref.shape[0]
    )
    repeat(far, lambda t: passed_landed(t).wait_recv())
    copy(partner, 2 * far, partner).wait_recv()
    repeat(far, lambda t: far_copy(t).wait_send())
    repeat(far, lambda t: pass_on(t).wait_send())
    copy(me, 2 * far, partner).wait_send()


def pair_kernel(
    node_buckets,
    count_ref,
    bucket_hbm,
    owner_hbm,
    slot_hbm,
    points_ref,
    geom_ref,
    wide_ref,
    nodes_ref,
    rows_ref,
    bucket_ref,
    owner_ref,
    slot_ref,
    load_sem,
    odd_ref,
    even_sum,
    odd_sum,
    even_part,
    odd_part,
):
    facet_buckets = geom_ref.shape[0]
    slots = bucket_ref.shape[0]
    loads = [
        pltpu.make_async_copy(src, dst, load_sem.at[i])
        for i, (src, dst) in enumerate(
            ((bucket_hbm, bucket_ref), (owner_hbm, owner_ref), (slot_hbm, slot_ref))
        )
    ]
    for load in loads:
        load.start()
    for ref in (nodes_ref, odd_ref, even_sum, odd_sum):
        ref[...] = jnp.zeros_like(ref)

    count = count_ref[0, 0]
    place = lax.broadcasted_iota(jnp.int32, (8, BUCKET), 0)
    blank = jnp.zeros((8, BUCKET), F32)
    one_or_zero = jnp.where(place == 4, 1.0, 0.0)
    spare = nodes_ref.shape[0] - 3 * node_buckets

    def base_of(p):
        return owner_ref[p] * (3 * node_buckets) + slot_ref[p]

    def products(p, part_ref):
        base = base_of(p)
        x, y, z = (
            jnp.broadcast_to(points_ref[pl.ds(base + k * node_buckets, 1), :], (8, BUCKET))
            for k in range(3)
        )
        square = x * x + y * y + z * z
        value = jnp.where(place == 3, square, one_or_zero)
        value = jnp.where(place == 2, z, value)
        value = jnp.where(place == 1, y, value)
        value = jnp.where(place == 0, x, value)
        v1, v2, v3 = split3(value)
        parts = [v1, v1, v1, v2, v2, v3]
        left = jnp.concatenate(parts + [blank] * 10, 0)
        right = jnp.concatenate([blank] * 6 + parts + [blank] * 4, 0)
        table = jnp.concatenate([left, right], 1).astype(BF16)
        part_ref[...] = jnp.dot(geom_ref[bucket_ref[p]], table, preferred_element_type=F32)

    def forces(p, part_ref, force_ref, sum_ref):
        live = p < count
        at = jnp.minimum(p, slots - 1)
        b = bucket_ref[at]
        minus_gap, fade = part_ref[:, :BUCKET], part_ref[:, BUCKET:]
        small = jnp.exp(-jnp.abs(minus_gap))
        logs = jnp.where(small < 2.0**-8, small * (1.0 - 0.5 * small), jnp.log(1.0 + small))
        strength = (jnp.maximum(minus_gap, 0.0) + logs) * jnp.exp2(fade)
        to_bucket = jnp.where(live, b, facet_buckets)
        to_node = jnp.where(live, base_of(at), spare)
        sum_ref[to_bucket] += strength
        for k in range(3):
            term = jnp.sum(wide_ref[b, k] * strength, axis=0, keepdims=True)
            force_ref[pl.ds(to_node + k * node_buckets, 1), :] += term

    for load in loads:
        load.wait()
    products(0, even_part)

    def step(i, carry):
        p = 2 * i
        last = slots - 1
        products(jnp.minimum(p + 1, last), odd_part)
        forces(p, even_part, nodes_ref, even_sum)
        products(jnp.minimum(p + 2, last), even_part)
        forces(p + 1, odd_part, odd_ref, odd_sum)
        return carry

    lax.fori_loop(0, lax.div(count + 1, 2), step, 0)

    nodes_ref[...] += odd_ref[...]
    for b in range(facet_buckets):
        rows_ref[b : b + 1, :] = jnp.sum((even_sum[b] + odd_sum[b]).T, axis=0, keepdims=True)


def spread(index, values, result):
    node_buckets = result.shape[0] // 6
    high_at = lax.broadcasted_iota(jnp.int32, (node_buckets, BUCKET), 0)
    low_at = lax.broadcasted_iota(jnp.int32, (BUCKET, BUCKET), 0)
    high = lax.div(index, BUCKET)
    low = index - high * BUCKET
    hit = high == high_at
    onehot = jnp.where(low == low_at, 1.0, 0.0).astype(BF16)
    firsts = [v.astype(BF16).astype(F32) for v in values]
    rests = [v - f for v, f in zip(values, firsts)]
    left = jnp.concatenate([jnp.where(hit, v, 0.0) for v in firsts + rests], 0)
    return result + lax.dot_general(
        left.astype(BF16), onehot, (((1,), (1,)), ((), ())), preferred_element_type=F32
    )


def exchange_kernel(
    domains,
    copies,
    nodes_ref,
    rows_ref,
    normal_ref,
    order_ref,
    corner_ref,
    out_ref,
    landed,
    total,
    landed_total,
    send_sem,
    recv_sem,
    send_total,
    recv_total,
):
    me = lax.axis_index("dom")
    rep = lax.axis_index("rep")
    size = landed.shape[1]
    node_buckets = size // 3
    facet_buckets = rows_ref.shape[0]
    barrier = pltpu.get_barrier_semaphore()

    def dom_peer(t):
        return across(me, domains - 1 - t, domains)

    def rep_peer(t):
        return lax.rem(rep + t + 1, copies)

    def signal(where):
        pl.semaphore_signal(barrier, inc=1, device_id=where, device_id_type=MESH_ID)

    repeat(domains - 1, lambda t: signal({"dom": dom_peer(t)}))
    repeat(copies - 1, lambda t: signal({"rep": rep_peer(t)}))
    pl.semaphore_wait(barrier, domains + copies - 2)

    def copy(src, dst, send, recv, where):
        return pltpu.make_async_remote_copy(
            src_ref=src,
            dst_ref=dst,
            send_sem=send,
            recv_sem=recv,
            device_id=where,
            device_id_type=MESH_ID,
        )

    def node_copy(t):
        block = nodes_ref.at[pl.ds(pl.multiple_of(dom_peer(t) * size, 8), size)]
        return copy(
            block, landed.at[t], send_sem.at[t], recv_sem.at[t], {"dom": dom_peer(t)}
        )

    def total_copy(t):
        return copy(
            total, landed_total.at[t], send_total.at[t], recv_total.at[t], {"rep": rep_peer(t)}
        )

    repeat(domains - 1, lambda t: node_copy(t).start())

    result = jnp.zeros((2 * size, BUCKET), F32)
    for b in range(facet_buckets):
        at = slice(b * BUCKET, (b + 1) * BUCKET)
        row = (-STIFFNESS / 3.0) * rows_ref[b : b + 1, :]
        values = [normal_ref[k : k + 1, at] * row for k in range(3)]
        for corner in range(3):
            result = spread(corner_ref[corner : corner + 1, at], values, result)

    repeat(domains - 1, lambda t: node_copy(t).wait_recv())
    mine = nodes_ref[pl.ds(pl.multiple_of(me * size, 8), size), :]
    if domains <= 16:
        for t in range(domains - 1):
            mine = mine + landed[t]
    else:
        mine = lax.fori_loop(0, domains - 1, lambda t, s: s + landed[t], mine)
    mine = STIFFNESS * mine
    for j in range(node_buckets):
        values = [
            mine[k * node_buckets + j : k * node_buckets + j + 1, :] for k in range(3)
        ]
        result = spread(order_ref[:, j * BUCKET : (j + 1) * BUCKET], values, result)
    force = result[:size] + result[size:]
    total[...] = force
    repeat(domains - 1, lambda t: node_copy(t).wait_send())
    repeat(copies - 1, lambda t: total_copy(t).start())
    repeat(copies - 1, lambda t: total_copy(t).wait_recv())
    for t in range(copies - 1):
        force = force + landed_total[t]
    for k in range(3):
        for h in range(node_buckets):
            i = k * node_buckets + h
            out_ref[k : k + 1, h * BUCKET : (h + 1) * BUCKET] = force[i : i + 1]
    repeat(copies - 1, lambda t: total_copy(t).wait_send())


def per_device(
    node_pos,
    node_order,
    facet_centroid,
    facet_normal,
    facet_nodes,
    pair_bucket,
    pair_owner,
    pair_slot,
    pair_count,
):
    domains = lax.axis_size("dom")
    copies = lax.axis_size("rep")
    node_buckets = node_pos.shape[1] // BUCKET
    facet_buckets = facet_centroid.shape[1] // BUCKET
    size = 3 * node_buckets
    dma = pltpu.SemaphoreType.DMA
    shape = jax.ShapeDtypeStruct

    points, geom, wide = pl.pallas_call(
        functools.partial(gather_kernel, domains),
        name="gather_points",
        out_shape=[
            shape((domains * size, BUCKET), F32),
            shape((facet_buckets, BUCKET, BUCKET), BF16),
            shape((facet_buckets, 3, BUCKET, BUCKET), F32),
        ],
        in_specs=[HBM] * 4,
        out_specs=[VMEM] * 3,
        scratch_shapes=[
            pltpu.VMEM(node_pos.shape, F32),
            pltpu.VMEM(node_order.shape, jnp.int32),
            pltpu.VMEM(facet_centroid.shape, F32),
            pltpu.VMEM(facet_normal.shape, F32),
            dma((4,)),
            dma((domains - 1,)),
            dma((domains - 1,)),
        ],
        compiler_params=pltpu.CompilerParams(
            collective_id=0, has_side_effects=True, vmem_limit_bytes=16 << 20
        ),
    )(node_pos, node_order, facet_centroid, facet_normal)

    nodes, rows = pl.pallas_call(
        functools.partial(pair_kernel, node_buckets),
        name="pair_forces",
        out_shape=[
            shape(((domains + 1) * size, BUCKET), F32),
            shape((facet_buckets, BUCKET), F32),
        ],
        in_specs=[SMEM] + [HBM] * 3 + [VMEM] * 3,
        out_specs=[VMEM] * 2,
        scratch_shapes=[
            pltpu.SMEM((pair_bucket.size,), jnp.int32),
            pltpu.SMEM((pair_bucket.size,), jnp.int32),
            pltpu.SMEM((pair_bucket.size,), jnp.int32),
            dma((3,)),
            pltpu.VMEM(((domains + 1) * size, BUCKET), F32),
            pltpu.VMEM((facet_buckets + 1, BUCKET, BUCKET), F32),
            pltpu.VMEM((facet_buckets + 1, BUCKET, BUCKET), F32),
            pltpu.VMEM((BUCKET, 2 * BUCKET), F32),
            pltpu.VMEM((BUCKET, 2 * BUCKET), F32),
        ],
        compiler_params=pltpu.CompilerParams(vmem_limit_bytes=32 << 20),
    )(
        pair_count,
        pair_bucket.reshape(-1),
        pair_owner.reshape(-1),
        pair_slot.reshape(-1),
        points,
        geom,
        wide,
    )

    return pl.pallas_call(
        functools.partial(exchange_kernel, domains, copies),
        name="exchange_forces",
        out_shape=shape(node_pos.shape, F32),
        in_specs=[VMEM] * 5,
        out_specs=VMEM,
        scratch_shapes=[
            pltpu.VMEM((domains - 1, size, BUCKET), F32),
            pltpu.VMEM((size, BUCKET), F32),
            pltpu.VMEM((copies - 1, size, BUCKET), F32),
            dma((domains - 1,)),
            dma((domains - 1,)),
            dma((copies - 1,)),
            dma((copies - 1,)),
        ],
        compiler_params=pltpu.CompilerParams(
            collective_id=1, has_side_effects=True, vmem_limit_bytes=16 << 20
        ),
    )(nodes, rows, facet_normal, node_order, facet_nodes)


def solution(mesh):
    placed = (
        P(None, "dom"),
        P("dom", None),
        P(None, "dom"),
        P(None, "dom"),
        P(None, "dom"),
        P("rep", "dom", None),
        P("rep", "dom", None, None),
        P("rep", "dom", None),
        P("rep", "dom"),
    )
    return jax.shard_map(
        per_device, mesh=mesh, in_specs=placed, out_specs=P(None, "dom"), check_vma=False
    )
```

```python
import functools

import jax
import jax.numpy as jnp
from jax import lax
from jax.experimental import pallas as pl
from jax.experimental.pallas import tpu as pltpu
from jax.sharding import PartitionSpec as P

BUCKET = 128
STIFFNESS = 0.125
RADIUS_SQ = 4.0
LOG2E = 1.4426950408889634
MESH_ID = pl.DeviceIdType.MESH
VMEM = pl.BlockSpec(memory_space=pltpu.VMEM)
SMEM = pl.BlockSpec(memory_space=pltpu.SMEM)
F32 = jnp.float32
BF16 = jnp.bfloat16


def repeat(count, body):
    if count <= 16:
        for i in range(count):
            body(i)
    else:
        def step(i, carry):
            body(i)
            return carry

        lax.fori_loop(0, count, step, 0)


def split3(value):
    first = value.astype(BF16).astype(F32)
    rest = value - first
    second = rest.astype(BF16).astype(F32)
    return first, second, rest - second


def facet_tables(table_ref, geom_ref, wide_ref):
    scale = LOG2E / RADIUS_SQ
    nothing = jnp.zeros((1, BUCKET), F32)

    def prepare(b, carry):
        at = pl.ds(pl.multiple_of(b * BUCKET, BUCKET), BUCKET)
        n = [table_ref[6 + k : 7 + k, at] for k in range(3)]
        c = [table_ref[3 + k : 4 + k, at] for k in range(3)]
        n_c = n[0] * c[0] + n[1] * c[1] + n[2] * c[2]
        c_c = c[0] * c[0] + c[1] * c[1] + c[2] * c[2]
        gap = jnp.concatenate([-n[0], -n[1], -n[2], nothing, n_c] + [nothing] * 3, 0)
        dist = jnp.concatenate(
            [2.0 * scale * c[0], 2.0 * scale * c[1], 2.0 * scale * c[2]]
            + [nothing - scale, -scale * c_c] + [nothing] * 3,
            0,
        )
        raw = jnp.concatenate(n + [nothing] * 5, 0)
        blank = jnp.zeros((BUCKET - 56, BUCKET), F32)
        for part, rows in enumerate((gap, dist)):
            a, bb, cc = split3(rows)
            table = jnp.concatenate([a, bb, cc, a, bb, a, raw, blank], 0).T
            geom_ref[b, part * BUCKET : (part + 1) * BUCKET, :] = table.astype(BF16)
            if part == 0:
                for k in range(3):
                    wide_ref[b, k] = jnp.broadcast_to(table[:, 48 + k : 49 + k], (BUCKET, BUCKET))
        return carry

    lax.fori_loop(0, geom_ref.shape[0], prepare, 0)


def gather_kernel(
    domains,
    table_ref,
    order_ref,
    out_ref,
    geom_ref,
    wide_ref,
    send_sem,
    recv_sem,
):
    me = lax.axis_index("dom")
    rows = out_ref.shape[0] // domains
    buckets = rows // 3
    barrier = pltpu.get_barrier_semaphore()

    def greet(t):
        peer = lax.rem(me + t + 1, domains)
        pl.semaphore_signal(barrier, inc=1, device_id={"dom": peer}, device_id_type=MESH_ID)

    repeat(domains - 1, greet)

    order = jnp.concatenate(
        [order_ref[:, h * BUCKET : (h + 1) * BUCKET] for h in range(buckets)], 0
    )
    high = lax.div(order, BUCKET)
    low = order - high * BUCKET
    own = pl.multiple_of(me * rows, 8)
    for k in range(3):
        picked = jnp.zeros((buckets, BUCKET), F32)
        for h in range(buckets):
            row = jnp.broadcast_to(
                table_ref[k : k + 1, h * BUCKET : (h + 1) * BUCKET], (buckets, BUCKET)
            )
            found = jnp.take_along_axis(row, low, axis=1, mode="promise_in_bounds")
            picked = jnp.where(high == h, found, picked)
        out_ref[pl.ds(own + k * buckets, buckets), :] = picked

    pl.semaphore_wait(barrier, domains - 1)
    block = out_ref.at[pl.ds(own, rows)]

    def copy_to(t):
        peer = lax.rem(me + t + 1, domains)
        return pltpu.make_async_remote_copy(
            src_ref=block,
            dst_ref=block,
            send_sem=send_sem.at[t],
            recv_sem=recv_sem.at[t],
            device_id={"dom": peer},
            device_id_type=MESH_ID,
        )

    def copy_from(t):
        source = lax.rem(me + 2 * domains - t - 1, domains)
        landed = out_ref.at[pl.ds(pl.multiple_of(source * rows, 8), rows)]
        return pltpu.make_async_remote_copy(
            src_ref=landed,
            dst_ref=landed,
            send_sem=send_sem.at[t],
            recv_sem=recv_sem.at[t],
            device_id={"dom": source},
            device_id_type=MESH_ID,
        )

    repeat(domains - 1, lambda t: copy_to(t).start())
    facet_tables(table_ref, geom_ref, wide_ref)
    repeat(domains - 1, lambda t: copy_from(t).wait_recv())
    repeat(domains - 1, lambda t: copy_to(t).wait_send())


def pair_kernel(
    node_buckets,
    count_ref,
    pair_ref,
    points_ref,
    geom_ref,
    wide_ref,
    nodes_ref,
    rows_ref,
    odd_ref,
    even_sum,
    odd_sum,
    even_part,
    odd_part,
):
    facet_buckets = geom_ref.shape[0]
    slots = pair_ref.shape[0]
    for ref in (nodes_ref, odd_ref, even_sum, odd_sum):
        ref[...] = jnp.zeros_like(ref)

    count = count_ref[0, 0]
    place = lax.broadcasted_iota(jnp.int32, (8, BUCKET), 0)
    blank = jnp.zeros((BUCKET - 48, BUCKET), F32)
    one_or_zero = jnp.where(place == 4, 1.0, 0.0)
    spare = nodes_ref.shape[0] - 3 * node_buckets

    def base_of(p):
        bucket = lax.div(pair_ref[p], facet_buckets)
        owner = lax.div(bucket, node_buckets)
        return owner * (3 * node_buckets) + (bucket - owner * node_buckets)

    def facets_of(p):
        return lax.rem(pair_ref[p], facet_buckets)

    def products(p, part_ref):
        base = base_of(p)
        x, y, z = (
            jnp.broadcast_to(points_ref[pl.ds(base + k * node_buckets, 1), :], (8, BUCKET))
            for k in range(3)
        )
        square = x * x + y * y + z * z
        value = jnp.where(place == 3, square, one_or_zero)
        value = jnp.where(place == 2, z, value)
        value = jnp.where(place == 1, y, value)
        value = jnp.where(place == 0, x, value)
        v1, v2, v3 = split3(value)
        table = jnp.concatenate([v1, v1, v1, v2, v2, v3, blank], 0).astype(BF16)
        part_ref[...] = jnp.dot(geom_ref[facets_of(p)], table, preferred_element_type=F32)

    def forces(p, part_ref, force_ref, sum_ref):
        live = p < count
        at = jnp.minimum(p, slots - 1)
        b = facets_of(at)
        minus_gap, fade = part_ref[:BUCKET], part_ref[BUCKET:]
        small = jnp.exp(-jnp.abs(minus_gap))
        logs = jnp.where(small < 2.0**-8, small * (1.0 - 0.5 * small), jnp.log(1.0 + small))
        strength = (jnp.maximum(minus_gap, 0.0) + logs) * jnp.exp2(fade)
        to_bucket = jnp.where(live, b, facet_buckets)
        to_node = jnp.where(live, base_of(at), spare)
        sum_ref[to_bucket] += strength
        for k in range(3):
            term = jnp.sum(wide_ref[b, k] * strength, axis=0, keepdims=True)
            force_ref[pl.ds(to_node + k * node_buckets, 1), :] += term

    products(0, even_part)

    def step(i, carry):
        p = 2 * i
        last = slots - 1
        products(jnp.minimum(p + 1, last), odd_part)
        forces(p, even_part, nodes_ref, even_sum)
        products(jnp.minimum(p + 2, last), even_part)
        forces(p + 1, odd_part, odd_ref, odd_sum)
        return carry

    lax.fori_loop(0, lax.div(count + 1, 2), step, 0)

    nodes_ref[...] += odd_ref[...]
    for b in range(facet_buckets):
        rows_ref[b : b + 1, :] = jnp.sum((even_sum[b] + odd_sum[b]).T, axis=0, keepdims=True)


def spread(index, values, result):
    node_buckets = result.shape[0] // 6
    high_at = lax.broadcasted_iota(jnp.int32, (node_buckets, BUCKET), 0)
    low_at = lax.broadcasted_iota(jnp.int32, (BUCKET, BUCKET), 0)
    high = lax.div(index, BUCKET)
    low = index - high * BUCKET
    hit = high == high_at
    onehot = jnp.where(low == low_at, 1.0, 0.0).astype(BF16)
    firsts = [v.astype(BF16).astype(F32) for v in values]
    rests = [v - f for v, f in zip(values, firsts)]
    left = jnp.concatenate([jnp.where(hit, v, 0.0) for v in firsts + rests], 0)
    return result + lax.dot_general(
        left.astype(BF16), onehot, (((1,), (1,)), ((), ())), preferred_element_type=F32
    )


def exchange_kernel(
    domains,
    copies,
    nodes_ref,
    rows_ref,
    normal_ref,
    order_ref,
    corner_ref,
    out_ref,
    landed,
    total,
    landed_total,
    send_sem,
    recv_sem,
    send_total,
    recv_total,
):
    me = lax.axis_index("dom")
    rep = lax.axis_index("rep")
    size = landed.shape[1]
    node_buckets = size // 3
    facet_buckets = rows_ref.shape[0]
    barrier = pltpu.get_barrier_semaphore()

    def dom_peer(t):
        return lax.rem(me + t + 1, domains)

    def rep_peer(t):
        return lax.rem(rep + t + 1, copies)

    def signal(where):
        pl.semaphore_signal(barrier, inc=1, device_id=where, device_id_type=MESH_ID)

    repeat(domains - 1, lambda t: signal({"dom": dom_peer(t)}))
    repeat(copies - 1, lambda t: signal({"rep": rep_peer(t)}))
    pl.semaphore_wait(barrier, domains + copies - 2)

    def copy(src, dst, send, recv, where):
        return pltpu.make_async_remote_copy(
            src_ref=src,
            dst_ref=dst,
            send_sem=send,
            recv_sem=recv,
            device_id=where,
            device_id_type=MESH_ID,
        )

    def node_copy(t):
        block = nodes_ref.at[pl.ds(pl.multiple_of(dom_peer(t) * size, 8), size)]
        return copy(
            block, landed.at[t], send_sem.at[t], recv_sem.at[t], {"dom": dom_peer(t)}
        )

    def total_copy(t):
        return copy(
            total, landed_total.at[t], send_total.at[t], recv_total.at[t], {"rep": rep_peer(t)}
        )

    repeat(domains - 1, lambda t: node_copy(t).start())

    result = jnp.zeros((2 * size, BUCKET), F32)
    for b in range(facet_buckets):
        at = slice(b * BUCKET, (b + 1) * BUCKET)
        row = (-STIFFNESS / 3.0) * rows_ref[b : b + 1, :]
        values = [normal_ref[k : k + 1, at] * row for k in range(3)]
        for corner in range(3):
            result = spread(corner_ref[corner : corner + 1, at], values, result)

    repeat(domains - 1, lambda t: node_copy(t).wait_recv())
    mine = nodes_ref[pl.ds(pl.multiple_of(me * size, 8), size), :]
    if domains <= 16:
        for t in range(domains - 1):
            mine = mine + landed[t]
    else:
        mine = lax.fori_loop(0, domains - 1, lambda t, s: s + landed[t], mine)
    mine = STIFFNESS * mine
    for j in range(node_buckets):
        values = [
            mine[k * node_buckets + j : k * node_buckets + j + 1, :] for k in range(3)
        ]
        result = spread(order_ref[:, j * BUCKET : (j + 1) * BUCKET], values, result)
    force = result[:size] + result[size:]
    total[...] = force
    repeat(domains - 1, lambda t: node_copy(t).wait_send())
    repeat(copies - 1, lambda t: total_copy(t).start())
    repeat(copies - 1, lambda t: total_copy(t).wait_recv())
    for t in range(copies - 1):
        force = force + landed_total[t]
    for k in range(3):
        for h in range(node_buckets):
            i = k * node_buckets + h
            out_ref[k : k + 1, h * BUCKET : (h + 1) * BUCKET] = force[i : i + 1]
    repeat(copies - 1, lambda t: total_copy(t).wait_send())


def per_device(
    node_pos,
    node_order,
    facet_centroid,
    facet_normal,
    facet_nodes,
    pair_bucket,
    pair_owner,
    pair_slot,
    pair_count,
):
    domains = lax.axis_size("dom")
    copies = lax.axis_size("rep")
    node_buckets = node_pos.shape[1] // BUCKET
    facet_buckets = facet_centroid.shape[1] // BUCKET
    size = 3 * node_buckets
    dma = pltpu.SemaphoreType.DMA
    shape = jax.ShapeDtypeStruct

    packed = pair_owner.reshape(-1) * node_buckets + pair_slot.reshape(-1)
    packed = packed * facet_buckets + pair_bucket.reshape(-1)

    points, geom, wide = pl.pallas_call(
        functools.partial(gather_kernel, domains),
        name="gather_points",
        out_shape=[
            shape((domains * size, BUCKET), F32),
            shape((facet_buckets, 2 * BUCKET, BUCKET), BF16),
            shape((facet_buckets, 3, BUCKET, BUCKET), F32),
        ],
        in_specs=[VMEM] * 2,
        out_specs=[VMEM] * 3,
        scratch_shapes=[dma((domains - 1,)), dma((domains - 1,))],
        compiler_params=pltpu.CompilerParams(
            collective_id=0, has_side_effects=True, vmem_limit_bytes=16 << 20
        ),
    )(jnp.concatenate([node_pos, facet_centroid, facet_normal], 0), node_order)

    nodes, rows = pl.pallas_call(
        functools.partial(pair_kernel, node_buckets),
        name="pair_forces",
        out_shape=[
            shape(((domains + 1) * size, BUCKET), F32),
            shape((facet_buckets, BUCKET), F32),
        ],
        in_specs=[SMEM] * 2 + [VMEM] * 3,
        out_specs=[VMEM] * 2,
        scratch_shapes=[
            pltpu.VMEM(((domains + 1) * size, BUCKET), F32),
            pltpu.VMEM((facet_buckets + 1, BUCKET, BUCKET), F32),
            pltpu.VMEM((facet_buckets + 1, BUCKET, BUCKET), F32),
            pltpu.VMEM((2 * BUCKET, BUCKET), F32),
            pltpu.VMEM((2 * BUCKET, BUCKET), F32),
        ],
        compiler_params=pltpu.CompilerParams(vmem_limit_bytes=32 << 20),
    )(
        pair_count,
        packed,
        points,
        geom,
        wide,
    )

    return pl.pallas_call(
        functools.partial(exchange_kernel, domains, copies),
        name="exchange_forces",
        out_shape=shape(node_pos.shape, F32),
        in_specs=[VMEM] * 5,
        out_specs=VMEM,
        scratch_shapes=[
            pltpu.VMEM((domains - 1, size, BUCKET), F32),
            pltpu.VMEM((size, BUCKET), F32),
            pltpu.VMEM((copies - 1, size, BUCKET), F32),
            dma((domains - 1,)),
            dma((domains - 1,)),
            dma((copies - 1,)),
            dma((copies - 1,)),
        ],
        compiler_params=pltpu.CompilerParams(
            collective_id=1, has_side_effects=True, vmem_limit_bytes=16 << 20
        ),
    )(nodes, rows, facet_normal, node_order, facet_nodes)


def solution(mesh):
    placed = (
        P(None, "dom"),
        P("dom", None),
        P(None, "dom"),
        P(None, "dom"),
        P(None, "dom"),
        P("rep", "dom", None),
        P("rep", "dom", None, None),
        P("rep", "dom", None),
        P("rep", "dom"),
    )
    return jax.shard_map(
        per_device, mesh=mesh, in_specs=placed, out_specs=P(None, "dom"), check_vma=False
    )
```
